32 devices in a mesh: ctx: 4 (over z), head: 8 (over y, x, core).
Axes of the slice: x: 2, y: 2, z: 4, core: 2. Of those that a mesh axis runs over, the one named last changes fastest.
Arguments:
- video: bfloat16 [3072, 4096], P('ctx', 'head'), may hold values from -6 to 6
- audio: bfloat16 [384, 2048], P('ctx', 'head'), may hold values from -6 to 6
- video_gain: float32 [4096], P('head'), may hold values from 0.1 to 1.9
- audio_gain: float32 [2048], P('head'), may hold values from 0.1 to 1.9
- video_qkv: bfloat16 [4096, 3, 4096], P(None, None, 'head'), as said below
- video_cross: bfloat16 [4096, 3, 2048], P(None, None, 'head'), as said below
- audio_cross: bfloat16 [2048, 3, 2048], P(None, None, 'head'), as said below
- video_out: bfloat16 [4096, 4096], P('head'), may hold values from -0.09375 to 0.09375
- cross_video_out: bfloat16 [2048, 4096], P('head'), may hold values from -0.125 to 0.125
- cross_audio_out: bfloat16 [2048, 2048], P('head'), may hold values from -0.125 to 0.125
Outputs:
- video_result: bfloat16 [3072, 4096], P('ctx', 'head')
- audio_result: bfloat16 [384, 2048], P('ctx', 'head')
The draws below stay inside these ranges and needn't reach their ends.
Inputs may be any that keep to these rules, and one draw needn't show every extreme that they name: `video_qkv`: entries lie within -32 / sqrt(4096) and 32 / sqrt(4096). `video_cross`: entries lie within -32 / sqrt(4096) and 32 / sqrt(4096). `audio_cross`: entries lie within -32 / sqrt(2048) and 32 / sqrt(2048).
All inputs are finite; a program needn't handle non-finite values.
Results may differ from the reference program's by a relative error of at most 0.014.
The reference program's roundings to bfloat16 on the way count: a program that leaves them out, or rounds other values in their place, can miss the bound.
Values may be sent and summed in bfloat16 or wider, within the bound.
A program may use at most 128 MiB of HBM per device.

```python
import jax
import jax.numpy as jnp
from jax import lax

DV = 4096
DA = 2048
DC = 2048
HD = 128
VTOK = 3072
ATOK = 384


def projection_draw(key, element_salt, heads_salt, rows, width):
    element_key = jax.random.fold_in(key, element_salt)
    heads = width // HD
    flags = (jax.random.permutation(jax.random.fold_in(key, heads_salt), heads) < max(1, heads // 4)).astype(jnp.float32)
    factor = 8.0
    base = jax.random.truncated_normal(element_key, -4.0, 4.0, (rows, 3, width), jnp.float32)
    columns = jnp.repeat(1.0 + (factor - 1.0) * flags, HD)
    blocks = jnp.array([1.0, 1.0, 0.0], jnp.float32)
    scaling = 1.0 + blocks[:, None] * (columns[None, :] - 1.0)
    return (base * scaling[None, :, :] * rows ** (-0.5)).astype(jnp.bfloat16)


def draw_video_qkv(key, part):
    return projection_draw(key, 11, 21, DV, DV)


def draw_video_cross(key, part):
    return projection_draw(key, 12, 22, DV, DC)


def draw_audio_cross(key, part):
    return projection_draw(key, 13, 22, DA, DC)


def level_of(own_key, shape, pieces, low, largest):
    loudness = 1.0
    for dim, shards_of in pieces:
        draws = jax.random.uniform(jax.random.fold_in(jax.random.fold_in(own_key, 6), dim), (shards_of,), jnp.float32, low / len(pieces), largest / len(pieces))
        loudness = loudness * jnp.repeat(jnp.exp(draws), shape[dim] // shards_of).reshape((-1,) + (1,) * (len(shape) - 1 - dim))
    return loudness


def bell_draw(own_key, dims, scale, most, pieces=(), held_as=jnp.bfloat16):
    values = scale * jax.random.normal(own_key, dims, jnp.float32)
    if pieces:
        values = values * level_of(own_key, dims, pieces, -0.22, 0.18)
    return jnp.clip(values, -most, most).astype(held_as)


def setup_inputs(seed: int = 0) -> dict:
    key_list = jax.random.split(jax.random.key(seed), 11)
    video = bell_draw(key_list[0], (VTOK, DV), 1.0, 6.0, ((0, 4), (1, 8)))
    audio = bell_draw(key_list[1], (ATOK, DA), 1.0, 6.0, ((0, 4), (1, 8)))
    video_gain = jnp.clip(1.0 + 0.18 * jax.random.normal(key_list[2], (DV,), jnp.float32), 0.1, 1.9)
    audio_gain = jnp.clip(1.0 + 0.18 * jax.random.normal(key_list[3], (DA,), jnp.float32), 0.1, 1.9)
    video_qkv = draw_video_qkv(jax.random.fold_in(key_list[10], 71), 0)
    video_cross = draw_video_cross(jax.random.fold_in(key_list[10], 71), 0)
    audio_cross = draw_audio_cross(jax.random.fold_in(key_list[10], 71), 0)
    video_out = bell_draw(key_list[7], (DV, DV), DV ** -0.5, 0.09375, ((0, 8),))
    cross_video_out = bell_draw(key_list[8], (DC, DV), DC ** -0.5, 0.125, ((0, 8),))
    cross_audio_out = bell_draw(key_list[9], (DC, DA), DC ** -0.5, 0.125, ((0, 8),))
    return dict(video=video, audio=audio, video_gain=video_gain, audio_gain=audio_gain, video_qkv=video_qkv, video_cross=video_cross, audio_cross=audio_cross, video_out=video_out, cross_video_out=cross_video_out, cross_audio_out=cross_audio_out)


EPSILON = 1e-06

def attend(queries, keys, values):
    heads = queries.shape[1] // HD
    scale = HD ** (-0.5)

    def split_heads(matrix):
        return matrix.reshape(matrix.shape[0], heads, HD).transpose(1, 0, 2)

    def one_head(operands):
        query_block, key_block, value_block = operands
        scores = jnp.dot(query_block, key_block.T, preferred_element_type=jnp.float32) * scale
        highest = lax.optimization_barrier(jnp.max(scores, axis=1, keepdims=True))
        weights = jnp.exp(scores - highest)
        totals = lax.optimization_barrier(jnp.sum(weights, axis=1, keepdims=True))
        return jnp.dot(weights.astype(jnp.bfloat16), value_block, preferred_element_type=jnp.float32) / totals
    blocks = lax.map(one_head, (split_heads(queries), split_heads(keys), split_heads(values)))
    return blocks.transpose(1, 0, 2).reshape(queries.shape[0], heads * HD).astype(jnp.bfloat16)

def reference(video, audio, video_gain, audio_gain, video_qkv, video_cross, audio_cross, video_out, cross_video_out, cross_audio_out):
    video_wide = video.astype(jnp.float32)
    audio_wide = audio.astype(jnp.float32)
    video_rate = lax.rsqrt(lax.optimization_barrier(jnp.sum(video_wide * video_wide, axis=1)) / DV + EPSILON)
    audio_rate = lax.rsqrt(lax.optimization_barrier(jnp.sum(audio_wide * audio_wide, axis=1)) / DA + EPSILON)
    video_scaled = (video_wide * video_gain).astype(jnp.bfloat16)
    audio_scaled = (audio_wide * audio_gain).astype(jnp.bfloat16)
    self_proj = (jnp.dot(video_scaled, video_qkv.reshape(DV, 3 * DV), preferred_element_type=jnp.float32) * video_rate[:, None]).astype(jnp.bfloat16)
    video_mixed = (jnp.dot(video_scaled, video_cross.reshape(DV, 3 * DC), preferred_element_type=jnp.float32) * video_rate[:, None]).astype(jnp.bfloat16)
    audio_mixed = (jnp.dot(audio_scaled, audio_cross.reshape(DA, 3 * DC), preferred_element_type=jnp.float32) * audio_rate[:, None]).astype(jnp.bfloat16)
    self_out = attend(self_proj[:, :DV], self_proj[:, DV:2 * DV], self_proj[:, 2 * DV:])
    video_cross_out = attend(video_mixed[:, :DC], audio_mixed[:, DC:2 * DC], audio_mixed[:, 2 * DC:])
    audio_cross_out = attend(audio_mixed[:, :DC], video_mixed[:, DC:2 * DC], video_mixed[:, 2 * DC:])
    video_sum = jnp.dot(self_out, video_out, preferred_element_type=jnp.float32) + jnp.dot(video_cross_out, cross_video_out, preferred_element_type=jnp.float32)
    audio_sum = jnp.dot(audio_cross_out, cross_audio_out, preferred_element_type=jnp.float32)
    return ((video_wide + video_sum).astype(jnp.bfloat16), (audio_wide + audio_sum).astype(jnp.bfloat16))
```

```python
import functools
import math

import jax
import jax.numpy as jnp
from jax import lax
from jax.experimental import pallas as pl
from jax.experimental.pallas import tpu as pltpu
from jax.sharding import PartitionSpec as P

HD = 128


EPSILON = 1e-06


def split_heads(matrix):
    return matrix.reshape(matrix.shape[0], -1, HD).transpose(1, 0, 2)


def join_heads(blocks):
    return blocks.transpose(1, 0, 2).reshape(blocks.shape[1], -1)


def attend(queries, keys, values):
    scale = HD ** (-0.5)

    def one_head(operands):
        query_block, key_block, value_block = operands
        scores = jnp.dot(query_block, key_block.T, preferred_element_type=jnp.float32) * scale
        highest = jnp.max(scores, axis=1, keepdims=True)
        weights = jnp.exp(scores - highest)
        totals = jnp.sum(weights, axis=1, keepdims=True)
        return (
            jnp.dot(weights.astype(jnp.bfloat16), value_block, preferred_element_type=jnp.float32)
            / totals
        )

    blocks = lax.map(one_head, (split_heads(queries), split_heads(keys), split_heads(values)))
    return join_heads(blocks).astype(jnp.bfloat16)


def plain_body(
    video,
    audio,
    video_gain,
    audio_gain,
    video_qkv,
    video_cross,
    audio_cross,
    video_out,
    cross_video_out,
    cross_audio_out,
):
    scale = HD ** (-0.5)
    video_wide = video.astype(jnp.float32)
    audio_wide = audio.astype(jnp.float32)
    video_squares, audio_squares = lax.psum(
        (jnp.sum(video_wide * video_wide, axis=1), jnp.sum(audio_wide * audio_wide, axis=1)), "head"
    )
    video_rate = lax.rsqrt(video_squares / video_qkv.shape[0] + EPSILON)
    audio_rate = lax.rsqrt(audio_squares / audio_cross.shape[0] + EPSILON)
    video_scaled = (video_wide * video_gain).astype(jnp.bfloat16)
    audio_scaled = (audio_wide * audio_gain).astype(jnp.bfloat16)
    self_weight = video_qkv.reshape(video_qkv.shape[0], -1)
    mixed_weight = video_cross.reshape(video_cross.shape[0], -1)
    audio_weight = audio_cross.reshape(audio_cross.shape[0], -1)
    self_width = video_qkv.shape[2]
    cross_width = video_cross.shape[2]
    video_rows = video.shape[0]
    segment = lax.all_gather(video_scaled, "head", axis=1, tiled=True)
    self_acc = jnp.dot(segment, self_weight, preferred_element_type=jnp.float32)
    mixed_acc = jnp.dot(segment, mixed_weight, preferred_element_type=jnp.float32)
    audio_acc = jnp.dot(
        lax.all_gather(audio_scaled, "head", axis=1, tiled=True),
        audio_weight,
        preferred_element_type=jnp.float32,
    )
    self_proj = (self_acc * video_rate[:, None]).astype(jnp.bfloat16)
    video_mixed = (mixed_acc * video_rate[:, None]).astype(jnp.bfloat16)
    audio_mixed = (audio_acc * audio_rate[:, None]).astype(jnp.bfloat16)
    query_heads = split_heads(self_proj[:, :self_width])
    local_heads = query_heads.shape[0]
    running_max = jnp.full((local_heads, video_rows), -1e30, jnp.float32)
    key_heads = split_heads(
        lax.all_gather(self_proj[:, self_width : 2 * self_width], "ctx", axis=0, tiled=True)
    )
    value_heads = split_heads(
        lax.all_gather(self_proj[:, 2 * self_width :], "ctx", axis=0, tiled=True)
    )
    scores = (
        jnp.einsum("hqd,hkd->hqk", query_heads, key_heads, preferred_element_type=jnp.float32)
        * scale
    )
    newest = jnp.maximum(running_max, jnp.max(scores, axis=2))
    weights = jnp.exp(scores - newest[:, :, None])
    running_sum = jnp.sum(weights, axis=2)
    running_acc = jnp.einsum(
        "hqk,hkd->hqd",
        weights.astype(jnp.bfloat16),
        value_heads,
        preferred_element_type=jnp.float32,
    )
    self_out = join_heads(running_acc / running_sum[:, :, None]).astype(jnp.bfloat16)
    audio_key_all, audio_value_all = (
        lax.all_gather(audio_mixed[:, cross_width : 2 * cross_width], "ctx", axis=0, tiled=True),
        lax.all_gather(audio_mixed[:, 2 * cross_width :], "ctx", axis=0, tiled=True),
    )
    video_cross_out = attend(video_mixed[:, :cross_width], audio_key_all, audio_value_all)
    queries_av = audio_mixed[:, :cross_width]
    keys_av = video_mixed[:, cross_width : 2 * cross_width]
    values_av = video_mixed[:, 2 * cross_width :]
    every_query = lax.all_gather(queries_av, "ctx", axis=0, tiled=True)
    scores = (
        jnp.einsum(
            "hqd,hkd->hqk",
            split_heads(every_query),
            split_heads(keys_av),
            preferred_element_type=jnp.float32,
        )
        * scale
    )
    highest = lax.pmax(jnp.max(scores, axis=2), "ctx")
    weights = jnp.exp(scores - highest[:, :, None])
    numerators = jnp.einsum(
        "hqk,hkd->hqd",
        weights.astype(jnp.bfloat16),
        split_heads(values_av),
        preferred_element_type=jnp.float32,
    )
    weight_totals = jnp.sum(weights, axis=2)
    own_numer, own_totals = (
        lax.psum_scatter(
            numerators.astype(jnp.bfloat16), "ctx", scatter_dimension=1, tiled=True
        ).astype(jnp.float32),
        lax.psum_scatter(
            weight_totals.astype(jnp.bfloat16), "ctx", scatter_dimension=1, tiled=True
        ).astype(jnp.float32),
    )
    audio_cross_out = join_heads(own_numer / own_totals[:, :, None]).astype(jnp.bfloat16)
    video_partial = jnp.dot(self_out, video_out, preferred_element_type=jnp.float32) + jnp.dot(
        video_cross_out, cross_video_out, preferred_element_type=jnp.float32
    )
    audio_partial = jnp.dot(audio_cross_out, cross_audio_out, preferred_element_type=jnp.float32)
    video_sum, audio_sum = (
        lax.psum_scatter(
            video_partial.astype(jnp.bfloat16), "head", scatter_dimension=1, tiled=True
        ).astype(jnp.float32),
        lax.psum_scatter(
            audio_partial.astype(jnp.bfloat16), "head", scatter_dimension=1, tiled=True
        ).astype(jnp.float32),
    )
    return (
        (video_wide + video_sum).astype(jnp.bfloat16),
        (audio_wide + audio_sum).astype(jnp.bfloat16),
    )


MESH = pl.DeviceIdType.MESH
F32 = jnp.float32
BF16 = jnp.bfloat16
VMEM_LIMIT = 60 * 1024 * 1024


def greet(peers):
    barrier = pltpu.get_barrier_semaphore()
    for peer in peers:
        pl.semaphore_signal(barrier, inc=1, device_id=peer, device_id_type=MESH)
    pl.semaphore_wait(barrier, len(peers))


def head_peer(me, flip):
    low = me % 2
    mid = (me // 2) % 2
    high = me // 4
    if flip & 1:
        low = 1 - low
    if flip & 2:
        mid = 1 - mid
    if flip & 4:
        high = 1 - high
    return high * 4 + mid * 2 + low


def half_rows(rows):
    return (rows // 2 + 15) // 16 * 16


def gather_kernel(x_ref, sq_ref, out_ref, sqs_ref, send, recv, own_sem):
    ctx = lax.axis_index("ctx")
    me = lax.axis_index("head")
    rows = x_ref.shape[0]
    half = half_rows(rows)
    top = pl.ds(0, half)
    low = pl.ds(half, rows - half)
    peer = [head_peer(me, flip) for flip in range(8)]
    greet([(ctx, peer[flip]) for flip in range(1, 8)])

    def copy(slot, flip, source, target):
        return pltpu.make_async_remote_copy(
            src_ref=source,
            dst_ref=target,
            send_sem=send.at[slot],
            recv_sem=recv.at[slot],
            device_id=(ctx, peer[flip]),
            device_id_type=MESH,
        )

    squares = [copy(10 + flip, flip, sq_ref, sqs_ref.at[flip]) for flip in range(1, 8)]
    x_top = copy(0, 2, x_ref.at[top], out_ref.at[me, top])
    x_low = copy(1, 2, x_ref.at[low], out_ref.at[me, low])
    y_low = copy(2, 4, x_ref.at[low], out_ref.at[me, low])
    y_top = copy(3, 4, x_ref.at[top], out_ref.at[me, top])
    side = copy(4, 1, x_ref, out_ref.at[me])
    x_top.start()
    y_low.start()
    x_low.start()
    y_top.start()
    for square in squares:
        square.start()
    side.start()
    own = pltpu.make_async_copy(x_ref, out_ref.at[me], own_sem.at[0])
    own_square = pltpu.make_async_copy(sq_ref, sqs_ref.at[0], own_sem.at[1])
    own.start()
    own_square.start()
    from_x = peer[2]
    from_y = peer[4]
    far = peer[6]
    x_top.wait_recv()
    far_top = copy(5, 4, out_ref.at[from_x, top], out_ref.at[from_x, top])
    far_top.start()
    y_low.wait_recv()
    far_low = copy(6, 2, out_ref.at[from_y, low], out_ref.at[from_y, low])
    far_low.start()
    x_low.wait_recv()
    side_x = copy(7, 1, out_ref.at[from_x], out_ref.at[from_x])
    side_x.start()
    y_top.wait_recv()
    side_y = copy(8, 1, out_ref.at[from_y], out_ref.at[from_y])
    side_y.start()
    far_top.wait_recv()
    side_top = copy(9, 1, out_ref.at[far, top], out_ref.at[far, top])
    side_top.start()
    far_low.wait_recv()
    side_low = copy(10, 1, out_ref.at[far, low], out_ref.at[far, low])
    side_low.start()
    for one in (side, side_x, side_y, side_top, side_low):
        one.wait_recv()
    for square in squares:
        square.wait_recv()
    own.wait()
    own_square.wait()
    for one in squares + [
        x_top, x_low, y_low, y_top, side, far_top, far_low, side_x, side_y, side_top, side_low
    ]:
        one.wait_send()


def gather_blocks(block, squares):
    return pl.pallas_call(
        gather_kernel,
        out_shape=(
            jax.ShapeDtypeStruct((8,) + block.shape, block.dtype),
            jax.ShapeDtypeStruct((8,) + squares.shape, squares.dtype),
        ),
        in_specs=[pl.BlockSpec(memory_space=pltpu.VMEM)] * 2,
        out_specs=(pl.BlockSpec(memory_space=pl.ANY), pl.BlockSpec(memory_space=pl.ANY)),
        scratch_shapes=[
            pltpu.SemaphoreType.DMA((18,)),
            pltpu.SemaphoreType.DMA((18,)),
            pltpu.SemaphoreType.DMA((2,)),
        ],
        compiler_params=pltpu.CompilerParams(collective_id=0, has_side_effects=True),
        name="gather_blocks",
    )(block, squares)


def scatter_kernel(part_ref, base_ref, out_ref, chip, x_in, y_in, x_last, y_last, send, recv):
    ctx = lax.axis_index("ctx")
    me = lax.axis_index("head")
    rows = base_ref.shape[0]
    half = half_rows(rows)
    top = pl.ds(0, half)
    low = pl.ds(half, rows - half)
    peer = [head_peer(me, flip) for flip in range(8)]
    greet([(ctx, peer[flip]) for flip in (1, 2, 4)])

    def copy(slot, flip, source, target):
        return pltpu.make_async_remote_copy(
            src_ref=source,
            dst_ref=target,
            send_sem=send.at[slot],
            recv_sem=recv.at[slot],
            device_id=(ctx, peer[flip]),
            device_id_type=MESH,
        )

    side = [copy(k, 1, part_ref.at[peer[2 * k + 1]], chip.at[k]) for k in range(4)]
    for k in (3, 1, 2, 0):
        side[k].start()

    def add_chip(k):
        side[k].wait_recv()
        chip[k] = (chip[k].astype(F32) + part_ref[peer[2 * k]].astype(F32)).astype(BF16)

    add_chip(3)
    x_far = copy(4, 2, chip.at[3, top], x_in.at[1])
    y_far = copy(5, 4, chip.at[3, low], y_in.at[1, pl.ds(0, rows - half)])
    x_far.start()
    y_far.start()
    add_chip(1)
    x_near = copy(6, 2, chip.at[1, top], x_in.at[0])
    x_near.start()
    add_chip(2)
    y_near = copy(7, 4, chip.at[2, low], y_in.at[0, pl.ds(0, rows - half)])
    y_near.start()
    side[0].wait_recv()
    x_far.wait_recv()
    chip[2, :half] = (chip[2, :half].astype(F32) + x_in[1].astype(F32)).astype(BF16)
    y_end = copy(8, 4, chip.at[2, top], y_last)
    y_end.start()
    y_far.wait_recv()
    chip[1, half:] = (
        chip[1, half:].astype(F32) + y_in[1, : rows - half].astype(F32)
    ).astype(BF16)
    x_end = copy(9, 2, chip.at[1, low], x_last.at[pl.ds(0, rows - half)])
    x_end.start()
    total = chip[0].astype(F32) + part_ref[me].astype(F32) + base_ref[...].astype(F32)
    x_near.wait_recv()
    y_near.wait_recv()
    total_top = total[:half] + x_in[0].astype(F32)
    total_low = total[half:] + y_in[0, : rows - half].astype(F32)
    y_end.wait_recv()
    out_ref[:half] = (total_top + y_last[...].astype(F32)).astype(BF16)
    x_end.wait_recv()
    out_ref[half:] = (total_low + x_last[: rows - half].astype(F32)).astype(BF16)
    for one in side + [x_far, y_far, x_near, y_near, y_end, x_end]:
        one.wait_send()


def scatter_blocks(parts, base):
    rows, width = base.shape
    half = half_rows(rows)
    return pl.pallas_call(
        scatter_kernel,
        out_shape=jax.ShapeDtypeStruct(base.shape, base.dtype),
        in_specs=[pl.BlockSpec(memory_space=pltpu.VMEM)] * 2,
        out_specs=pl.BlockSpec(memory_space=pltpu.VMEM),
        scratch_shapes=[
            pltpu.VMEM((4, rows, width), BF16),
            pltpu.VMEM((2, half, width), BF16),
            pltpu.VMEM((2, half, width), BF16),
            pltpu.VMEM((half, width), BF16),
            pltpu.VMEM((half, width), BF16),
            pltpu.SemaphoreType.DMA((10,)),
            pltpu.SemaphoreType.DMA((10,)),
        ],
        compiler_params=pltpu.CompilerParams(
            collective_id=1, has_side_effects=True, vmem_limit_bytes=VMEM_LIMIT
        ),
        name="scatter_blocks",
    )(parts, base)


def project_kernel(heads, x_ref, w_ref, rate_ref, out_ref, total):
    step = pl.program_id(0)
    for plane in range(w_ref.shape[0]):
        product = jnp.dot(x_ref[0], w_ref[plane], preferred_element_type=F32)

        @pl.when(step == 0)
        def _():
            total[plane] = product

        @pl.when(step > 0)
        def _():
            total[plane] += product

    @pl.when(step == pl.num_programs(0) - 1)
    def _():
        for plane in range(w_ref.shape[0]):
            for h in range(heads):
                out_ref[h, plane] = (
                    total[plane, :, h * HD : (h + 1) * HD] * rate_ref[...]
                ).astype(BF16)


def project(blocks, rows, weight, rate):
    planes, _, width = weight.shape
    depth = blocks.shape[2]
    heads = width // HD
    return pl.pallas_call(
        functools.partial(project_kernel, heads),
        grid=(blocks.shape[0],),
        out_shape=jax.ShapeDtypeStruct((heads, planes, rows, HD), BF16),
        in_specs=[
            pl.BlockSpec((1, rows, depth), lambda b: (b, 0, 0)),
            pl.BlockSpec((planes, depth, width), lambda b: (0, b, 0)),
            pl.BlockSpec((rows, 1), lambda b: (0, 0)),
        ],
        out_specs=pl.BlockSpec((heads, planes, rows, HD), lambda b: (0, 0, 0, 0)),
        scratch_shapes=[pltpu.VMEM((planes, rows, width), F32)],
        compiler_params=pltpu.CompilerParams(
            dimension_semantics=("arbitrary",), vmem_limit_bytes=VMEM_LIMIT
        ),
        cost_estimate=pl.CostEstimate(
            flops=2 * planes * rows * width * depth * blocks.shape[0],
            bytes_accessed=2 * planes * width * depth * blocks.shape[0],
            transcendentals=0,
        ),
        name="project",
    )(blocks, weight, rate)


def contract_last(left, right):
    return lax.dot_general(left, right, (((1,), (1,)), ((), ())), preferred_element_type=F32)


def softmax_parts(query, keys, values):
    scale = HD ** (-0.5)
    scores = [contract_last(query, key) for key in keys]
    highest = functools.reduce(
        jnp.maximum, [jnp.max(score, axis=1, keepdims=True) for score in scores]
    )
    total = 0.0
    mixed = 0.0
    for score, value in zip(scores, values):
        weight = jnp.exp((score - highest) * scale)
        total = total + jnp.sum(weight, axis=1, keepdims=True)
        mixed = mixed + jnp.dot(weight.astype(BF16), value, preferred_element_type=F32)
    return mixed, total, highest * scale


def attention_kernel(count, q_ref, *refs):
    out_ref = refs[-1]
    keys = [refs[i][0, 0] for i in range(count)]
    values = [refs[count + i][0, 0] for i in range(count)]
    mixed, total, _ = softmax_parts(q_ref[0, 0], keys, values)
    out_ref[0] = (mixed / total).astype(BF16)


def self_attention(queries, sources):
    heads, _, rows, _ = queries.shape
    tile = math.gcd(rows, 256)
    count = len(sources)
    keys_all = count * rows
    return pl.pallas_call(
        functools.partial(attention_kernel, count),
        grid=(heads, rows // tile),
        out_shape=jax.ShapeDtypeStruct((heads, rows, HD), BF16),
        in_specs=[pl.BlockSpec((1, 1, tile, HD), lambda h, i: (h, 0, i, 0))]
        + [pl.BlockSpec((1, 1, rows, HD), lambda h, i: (h, 1, 0, 0))] * count
        + [pl.BlockSpec((1, 1, rows, HD), lambda h, i: (h, 2, 0, 0))] * count,
        out_specs=pl.BlockSpec((1, tile, HD), lambda h, i: (h, i, 0)),
        compiler_params=pltpu.CompilerParams(
            dimension_semantics=("arbitrary", "arbitrary"), vmem_limit_bytes=VMEM_LIMIT
        ),
        cost_estimate=pl.CostEstimate(
            flops=8 * heads * rows * keys_all * HD,
            bytes_accessed=4 * heads * keys_all * HD,
            transcendentals=heads * rows * keys_all,
        ),
        name="self_attention",
    )(queries, *sources, *sources)


def cross_kernel(count, video_ref, *refs):
    audio = refs[:count]
    out_ref, part_ref, stats_ref = refs[count:]
    heads = video_ref.shape[0]
    for h in range(heads):
        at = [slice((plane * heads + h) * HD, (plane * heads + h + 1) * HD) for plane in range(3)]
        mixed, total, _ = softmax_parts(
            video_ref[h, 0], [one[:, at[1]] for one in audio], [one[:, at[2]] for one in audio]
        )
        out_ref[:, h * HD : (h + 1) * HD] = (mixed / total).astype(BF16)
        for d in range(count):
            mixed, total, highest = softmax_parts(
                audio[d][:, at[0]], [video_ref[h, 1]], [video_ref[h, 2]]
            )
            part_ref[d, :, h * HD : (h + 1) * HD] = (mixed / total).astype(BF16)
            lanes = lax.broadcasted_iota(jnp.int32, (mixed.shape[0], HD), 1)
            stats_ref[d, h] = jnp.where(lanes < HD // 2, total, highest)


def cross_attention(video_heads, audio_sources):
    heads, _, rows, _ = video_heads.shape
    count = len(audio_sources)
    audio_rows = audio_sources[0].shape[0]
    whole = pl.BlockSpec(memory_space=pltpu.VMEM)
    return pl.pallas_call(
        functools.partial(cross_kernel, count),
        out_shape=(
            jax.ShapeDtypeStruct((rows, heads * HD), BF16),
            jax.ShapeDtypeStruct((count, audio_rows, heads * HD), BF16),
            jax.ShapeDtypeStruct((count, heads, audio_rows, HD), F32),
        ),
        in_specs=[whole] * (1 + count),
        out_specs=(whole, whole, whole),
        compiler_params=pltpu.CompilerParams(vmem_limit_bytes=VMEM_LIMIT),
        cost_estimate=pl.CostEstimate(
            flops=16 * heads * rows * count * audio_rows * HD,
            bytes_accessed=8 * rows * heads * HD,
            transcendentals=2 * heads * rows * count * audio_rows,
        ),
        name="cross_attention",
    )(video_heads, *audio_sources)


def output_kernel(self_ref, cross_ref, audio_ref, w_self, w_cross, w_audio, out_ref):
    rows = self_ref.shape[0]
    out_ref[0, :rows] = (
        jnp.dot(self_ref[...], w_self[...], preferred_element_type=F32)
        + jnp.dot(cross_ref[...], w_cross[...], preferred_element_type=F32)
    ).astype(BF16)
    sound = jnp.dot(audio_ref[...], w_audio[...], preferred_element_type=F32).astype(BF16)
    half = sound.shape[0] // 2
    width = sound.shape[1]
    out_ref[0, rows:, :width] = sound[:half]
    out_ref[0, rows:, width:] = sound[half:]


def output_parts(self_out, cross_out, audio_out, w_self, w_cross, w_audio):
    rows, depth = self_out.shape
    audio_rows, cross_depth = audio_out.shape
    width = w_self.shape[1] // 8
    audio_width = w_audio.shape[1] // 8
    return pl.pallas_call(
        output_kernel,
        grid=(8,),
        out_shape=jax.ShapeDtypeStruct((8, rows + audio_rows // 2, width), BF16),
        in_specs=[
            pl.BlockSpec((rows, depth), lambda n: (0, 0)),
            pl.BlockSpec((rows, cross_depth), lambda n: (0, 0)),
            pl.BlockSpec((audio_rows, cross_depth), lambda n: (0, 0)),
            pl.BlockSpec((depth, width), lambda n: (0, n)),
            pl.BlockSpec((cross_depth, width), lambda n: (0, n)),
            pl.BlockSpec((cross_depth, audio_width), lambda n: (0, n)),
        ],
        out_specs=pl.BlockSpec((1, rows + audio_rows // 2, width), lambda n: (n, 0, 0)),
        compiler_params=pltpu.CompilerParams(
            dimension_semantics=("arbitrary",), vmem_limit_bytes=VMEM_LIMIT
        ),
        name="output_parts",
    )(self_out, cross_out, audio_out, w_self, w_cross, w_audio)


def pack(video_block, audio_block):
    half = audio_block.shape[0] // 2
    return jnp.concatenate(
        [video_block, jnp.concatenate([audio_block[:half], audio_block[half:]], axis=1)], axis=0
    )


def square_tile(video_squares, audio_squares):
    flat = jnp.concatenate([video_squares, audio_squares])
    size = (flat.shape[0] + 1023) // 1024 * 1024
    return jnp.pad(flat, (0, size - flat.shape[0])).reshape(-1, 128)


def fast_body(
    ctx_size,
    video,
    audio,
    video_gain,
    audio_gain,
    video_qkv,
    video_cross,
    audio_cross,
    video_out,
    cross_video_out,
    cross_audio_out,
):
    me = lax.axis_index("ctx")
    rows = video.shape[0]
    audio_rows = audio.shape[0]

    def shift(value, distance):
        ring = [(i, (i + distance) % ctx_size) for i in range(ctx_size)]
        return lax.ppermute(value, "ctx", ring)

    video_wide = video.astype(F32)
    audio_wide = audio.astype(F32)
    block = pack((video_wide * video_gain).astype(BF16), (audio_wide * audio_gain).astype(BF16))
    squares = square_tile(
        jnp.sum(video_wide * video_wide, axis=1), jnp.sum(audio_wide * audio_wide, axis=1)
    )
    blocks, every_square = gather_blocks(block, squares)
    sums = jnp.sum(every_square, axis=0).reshape(-1)
    video_rate = lax.rsqrt(sums[:rows] / video_qkv.shape[0] + EPSILON)[:, None]
    audio_rate = lax.rsqrt(sums[rows : rows + audio_rows] / audio_cross.shape[0] + EPSILON)[:, None]

    self_heads = project(blocks, rows, video_qkv.transpose(1, 0, 2), video_rate)
    heads = self_heads.shape[0]
    shares = self_heads.reshape((ctx_size, heads // ctx_size) + self_heads.shape[1:])

    def share(stack, distance):
        return lax.dynamic_index_in_dim(stack, (me + distance) % ctx_size, 0, keepdims=False)

    sources = [share(shares, 0)] + [shift(share(shares, d), d) for d in range(1, ctx_size)]

    audio_full = (
        blocks[:, rows:, :]
        .reshape(8, audio_rows // 2, 2, -1)
        .transpose(2, 1, 0, 3)
        .reshape(audio_rows, -1)
    )
    audio_mixed = jnp.concatenate(
        [
            (
                jnp.dot(audio_full, audio_cross[:, plane, :], preferred_element_type=F32)
                * audio_rate
            ).astype(BF16)
            for plane in range(3)
        ],
        axis=1,
    )
    audio_sources = [audio_mixed] + [shift(audio_mixed, d) for d in range(1, ctx_size)]
    cross_heads = project(blocks, rows, video_cross.transpose(1, 0, 2), video_rate)
    cross_out, parts, stats = cross_attention(cross_heads, audio_sources)
    own_parts = jnp.stack([parts[0]] + [shift(parts[d], -d) for d in range(1, ctx_size)])
    stats = jnp.stack([stats[..., 0], stats[..., HD - 1]], axis=1)
    own_stats = jnp.stack([stats[0]] + [shift(stats[d], -d) for d in range(1, ctx_size)])
    totals, highs = own_stats[:, 0], own_stats[:, 1]
    shares_of = totals * jnp.exp(highs - jnp.max(highs, axis=0, keepdims=True))
    shares_of = (shares_of / jnp.sum(shares_of, axis=0, keepdims=True)).transpose(0, 2, 1)
    split_parts = own_parts.astype(F32).reshape(ctx_size, audio_rows, -1, HD)
    audio_cross_out = (
        jnp.sum(split_parts * shares_of[..., None], axis=0).reshape(audio_rows, -1).astype(BF16)
    )

    results = [None] * ctx_size
    for d in list(range(1, ctx_size)) + [0]:
        result = self_attention(sources[d], sources)
        results[d] = shift(result, -d) if d else result
    doubled = jnp.concatenate(results + results, axis=0)
    group = heads // ctx_size
    ordered = lax.dynamic_slice_in_dim(
        doubled, ((ctx_size - me) % ctx_size) * group, heads, axis=0
    )
    self_out = join_heads(ordered)
    partial = output_parts(
        self_out, cross_out, audio_cross_out, video_out, cross_video_out, cross_audio_out
    )
    done = scatter_blocks(partial, pack(video, audio))
    sound = done[rows:]
    width = audio.shape[1]
    return done[:rows], jnp.concatenate([sound[:, :width], sound[:, width:]], axis=0)


def solution(mesh):
    ctx_size = mesh.shape["ctx"]

    def body(*operands):
        heads = operands[4].shape[2] // HD
        if mesh.shape["head"] == 2**3 and heads % ctx_size == 0:
            return fast_body(ctx_size, *operands)
        return plain_body(*operands)

    return jax.shard_map(
        body,
        mesh=mesh,
        in_specs=(
            P("ctx", "head"),
            P("ctx", "head"),
            P("head"),
            P("head"),
            P(None, None, "head"),
            P(None, None, "head"),
            P(None, None, "head"),
            P("head", None),
            P("head", None),
            P("head", None),
        ),
        out_specs=(P("ctx", "head"), P("ctx", "head")),
        check_vma=False,
    )
```

```python
import functools
import math

import jax
import jax.numpy as jnp
from jax import lax
from jax.experimental import pallas as pl
from jax.experimental.pallas import tpu as pltpu
from jax.sharding import PartitionSpec as P

HD = 128


EPSILON = 1e-06


def split_heads(matrix):
    return matrix.reshape(matrix.shape[0], -1, HD).transpose(1, 0, 2)


def join_heads(blocks):
    return blocks.transpose(1, 0, 2).reshape(blocks.shape[1], -1)


def attend(queries, keys, values):
    scale = HD ** (-0.5)

    def one_head(operands):
        query_block, key_block, value_block = operands
        scores = jnp.dot(query_block, key_block.T, preferred_element_type=jnp.float32) * scale
        highest = jnp.max(scores, axis=1, keepdims=True)
        weights = jnp.exp(scores - highest)
        totals = jnp.sum(weights, axis=1, keepdims=True)
        return (
            jnp.dot(weights.astype(jnp.bfloat16), value_block, preferred_element_type=jnp.float32)
            / totals
        )

    blocks = lax.map(one_head, (split_heads(queries), split_heads(keys), split_heads(values)))
    return join_heads(blocks).astype(jnp.bfloat16)


def plain_body(
    video,
    audio,
    video_gain,
    audio_gain,
    video_qkv,
    video_cross,
    audio_cross,
    video_out,
    cross_video_out,
    cross_audio_out,
):
    scale = HD ** (-0.5)
    video_wide = video.astype(jnp.float32)
    audio_wide = audio.astype(jnp.float32)
    video_squares, audio_squares = lax.psum(
        (jnp.sum(video_wide * video_wide, axis=1), jnp.sum(audio_wide * audio_wide, axis=1)), "head"
    )
    video_rate = lax.rsqrt(video_squares / video_qkv.shape[0] + EPSILON)
    audio_rate = lax.rsqrt(audio_squares / audio_cross.shape[0] + EPSILON)
    video_scaled = (video_wide * video_gain).astype(jnp.bfloat16)
    audio_scaled = (audio_wide * audio_gain).astype(jnp.bfloat16)
    self_weight = video_qkv.reshape(video_qkv.shape[0], -1)
    mixed_weight = video_cross.reshape(video_cross.shape[0], -1)
    audio_weight = audio_cross.reshape(audio_cross.shape[0], -1)
    self_width = video_qkv.shape[2]
    cross_width = video_cross.shape[2]
    video_rows = video.shape[0]
    segment = lax.all_gather(video_scaled, "head", axis=1, tiled=True)
    self_acc = jnp.dot(segment, self_weight, preferred_element_type=jnp.float32)
    mixed_acc = jnp.dot(segment, mixed_weight, preferred_element_type=jnp.float32)
    audio_acc = jnp.dot(
        lax.all_gather(audio_scaled, "head", axis=1, tiled=True),
        audio_weight,
        preferred_element_type=jnp.float32,
    )
    self_proj = (self_acc * video_rate[:, None]).astype(jnp.bfloat16)
    video_mixed = (mixed_acc * video_rate[:, None]).astype(jnp.bfloat16)
    audio_mixed = (audio_acc * audio_rate[:, None]).astype(jnp.bfloat16)
    query_heads = split_heads(self_proj[:, :self_width])
    local_heads = query_heads.shape[0]
    running_max = jnp.full((local_heads, video_rows), -1e30, jnp.float32)
    key_heads = split_heads(
        lax.all_gather(self_proj[:, self_width : 2 * self_width], "ctx", axis=0, tiled=True)
    )
    value_heads = split_heads(
        lax.all_gather(self_proj[:, 2 * self_width :], "ctx", axis=0, tiled=True)
    )
    scores = (
        jnp.einsum("hqd,hkd->hqk", query_heads, key_heads, preferred_element_type=jnp.float32)
        * scale
    )
    newest = jnp.maximum(running_max, jnp.max(scores, axis=2))
    weights = jnp.exp(scores - newest[:, :, None])
    running_sum = jnp.sum(weights, axis=2)
    running_acc = jnp.einsum(
        "hqk,hkd->hqd",
        weights.astype(jnp.bfloat16),
        value_heads,
        preferred_element_type=jnp.float32,
    )
    self_out = join_heads(running_acc / running_sum[:, :, None]).astype(jnp.bfloat16)
    audio_key_all, audio_value_all = (
        lax.all_gather(audio_mixed[:, cross_width : 2 * cross_width], "ctx", axis=0, tiled=True),
        lax.all_gather(audio_mixed[:, 2 * cross_width :], "ctx", axis=0, tiled=True),
    )
    video_cross_out = attend(video_mixed[:, :cross_width], audio_key_all, audio_value_all)
    queries_av = audio_mixed[:, :cross_width]
    keys_av = video_mixed[:, cross_width : 2 * cross_width]
    values_av = video_mixed[:, 2 * cross_width :]
    every_query = lax.all_gather(queries_av, "ctx", axis=0, tiled=True)
    scores = (
        jnp.einsum(
            "hqd,hkd->hqk",
            split_heads(every_query),
            split_heads(keys_av),
            preferred_element_type=jnp.float32,
        )
        * scale
    )
    highest = lax.pmax(jnp.max(scores, axis=2), "ctx")
    weights = jnp.exp(scores - highest[:, :, None])
    numerators = jnp.einsum(
        "hqk,hkd->hqd",
        weights.astype(jnp.bfloat16),
        split_heads(values_av),
        preferred_element_type=jnp.float32,
    )
    weight_totals = jnp.sum(weights, axis=2)
    own_numer, own_totals = (
        lax.psum_scatter(
            numerators.astype(jnp.bfloat16), "ctx", scatter_dimension=1, tiled=True
        ).astype(jnp.float32),
        lax.psum_scatter(
            weight_totals.astype(jnp.bfloat16), "ctx", scatter_dimension=1, tiled=True
        ).astype(jnp.float32),
    )
    audio_cross_out = join_heads(own_numer / own_totals[:, :, None]).astype(jnp.bfloat16)
    video_partial = jnp.dot(self_out, video_out, preferred_element_type=jnp.float32) + jnp.dot(
        video_cross_out, cross_video_out, preferred_element_type=jnp.float32
    )
    audio_partial = jnp.dot(audio_cross_out, cross_audio_out, preferred_element_type=jnp.float32)
    video_sum, audio_sum = (
        lax.psum_scatter(
            video_partial.astype(jnp.bfloat16), "head", scatter_dimension=1, tiled=True
        ).astype(jnp.float32),
        lax.psum_scatter(
            audio_partial.astype(jnp.bfloat16), "head", scatter_dimension=1, tiled=True
        ).astype(jnp.float32),
    )
    return (
        (video_wide + video_sum).astype(jnp.bfloat16),
        (audio_wide + audio_sum).astype(jnp.bfloat16),
    )


MESH = pl.DeviceIdType.MESH
F32 = jnp.float32
BF16 = jnp.bfloat16
VMEM_LIMIT = 60 * 1024 * 1024


def greet(peers):
    barrier = pltpu.get_barrier_semaphore()
    for peer in peers:
        pl.semaphore_signal(barrier, inc=1, device_id=peer, device_id_type=MESH)
    pl.semaphore_wait(barrier, len(peers))


def head_peer(me, flip):
    low = me % 2
    mid = (me // 2) % 2
    high = me // 4
    if flip & 1:
        low = 1 - low
    if flip & 2:
        mid = 1 - mid
    if flip & 4:
        high = 1 - high
    return high * 4 + mid * 2 + low


def half_rows(rows):
    return (rows // 2 + 15) // 16 * 16


def gather_kernel(
    x_ref, sq_ref, w_ref, out_ref, sqs_ref, heads_ref, total, weights, send, recv, load
):
    ctx = lax.axis_index("ctx")
    me = lax.axis_index("head")
    rows = x_ref.shape[0]
    half = half_rows(rows)
    top = pl.ds(0, half)
    low = pl.ds(half, rows - half)
    peer = [head_peer(me, flip) for flip in range(8)]
    order = (0, 1, 2, 4, 3, 5, 6, 7)
    loads = {
        flip: pltpu.make_async_copy(w_ref.at[:, peer[flip]], weights.at[:, peer[flip]], load.at[flip])
        for flip in order
    }
    for flip in order:
        loads[flip].start()
    greet([(ctx, peer[flip]) for flip in range(1, 8)])

    def copy(slot, flip, source, target):
        return pltpu.make_async_remote_copy(
            src_ref=source,
            dst_ref=target,
            send_sem=send.at[slot],
            recv_sem=recv.at[slot],
            device_id=(ctx, peer[flip]),
            device_id_type=MESH,
        )

    squares = [copy(10 + flip, flip, sq_ref, sqs_ref.at[flip]) for flip in range(1, 8)]
    x_top = copy(0, 2, x_ref.at[top], out_ref.at[me, top])
    x_low = copy(1, 2, x_ref.at[low], out_ref.at[me, low])
    y_low = copy(2, 4, x_ref.at[low], out_ref.at[me, low])
    y_top = copy(3, 4, x_ref.at[top], out_ref.at[me, top])
    side = copy(4, 1, x_ref, out_ref.at[me])
    x_top.start()
    y_low.start()
    x_low.start()
    y_top.start()
    side.start()
    for square in squares:
        square.start()

    planes, tokens, width = total.shape
    tile = math.gcd(tokens, 256)
    tiles = tokens // tile

    def multiply(flip):
        loads[flip].wait()

        def step(i, carry):
            plane = i // tiles
            at = pl.ds(pl.multiple_of((i % tiles) * tile, tile), tile)
            product = jnp.dot(
                out_ref[peer[flip], at], weights[plane, peer[flip]], preferred_element_type=F32
            )
            total[plane, at] = product if flip == 0 else total[plane, at] + product
            return carry

        lax.fori_loop(0, planes * tiles, step, 0)

    out_ref[me] = x_ref[...]
    sqs_ref[0] = sq_ref[...]
    multiply(0)
    side.wait_recv()
    multiply(1)
    from_x = peer[2]
    from_y = peer[4]
    far = peer[6]
    x_top.wait_recv()
    far_top = copy(5, 4, out_ref.at[from_x, top], out_ref.at[from_x, top])
    far_top.start()
    y_low.wait_recv()
    far_low = copy(6, 2, out_ref.at[from_y, low], out_ref.at[from_y, low])
    far_low.start()
    x_low.wait_recv()
    side_x = copy(7, 1, out_ref.at[from_x], out_ref.at[from_x])
    side_x.start()
    y_top.wait_recv()
    side_y = copy(8, 1, out_ref.at[from_y], out_ref.at[from_y])
    side_y.start()
    multiply(2)
    multiply(4)
    side_x.wait_recv()
    multiply(3)
    far_top.wait_recv()
    side_top = copy(9, 1, out_ref.at[far, top], out_ref.at[far, top])
    side_top.start()
    far_low.wait_recv()
    side_low = copy(10, 1, out_ref.at[far, low], out_ref.at[far, low])
    side_low.start()
    side_y.wait_recv()
    multiply(5)
    multiply(6)
    side_top.wait_recv()
    side_low.wait_recv()
    multiply(7)
    for square in squares:
        square.wait_recv()
    sums = jnp.sum(sqs_ref[...], axis=0)
    rate_rows = lax.rsqrt(sums / (8 * x_ref.shape[1]) + EPSILON)
    line = lax.broadcasted_iota(jnp.int32, (HD, HD), 0)
    lane = lax.broadcasted_iota(jnp.int32, (HD, HD), 1)
    for piece in range(tokens // HD):
        spread = jnp.broadcast_to(rate_rows[piece : piece + 1], (HD, HD))
        rate = jnp.sum(jnp.where(line == lane, spread, 0.0), axis=1, keepdims=True)
        at = slice(piece * HD, (piece + 1) * HD)
        for plane in range(planes):
            scaled = (total[plane, at] * rate).astype(BF16)
            for h in range(width // HD):
                heads_ref[h, plane, at] = scaled[:, h * HD : (h + 1) * HD]
    for one in squares + [
        x_top, x_low, y_low, y_top, side, far_top, far_low, side_x, side_y, side_top, side_low
    ]:
        one.wait_send()


def gather_project(block, squares, weight, tokens):
    planes, depth, width = weight.shape
    vmem = pl.BlockSpec(memory_space=pltpu.VMEM)
    blocked = weight.reshape(planes, 8, depth // 8, width)
    return pl.pallas_call(
        gather_kernel,
        out_shape=(
            jax.ShapeDtypeStruct((8,) + block.shape, block.dtype),
            jax.ShapeDtypeStruct((8,) + squares.shape, squares.dtype),
            jax.ShapeDtypeStruct((width // HD, planes, tokens, HD), BF16),
        ),
        in_specs=[vmem, vmem, pl.BlockSpec(memory_space=pl.ANY)],
        out_specs=(vmem, vmem, vmem),
        scratch_shapes=[
            pltpu.VMEM((planes, tokens, width), F32),
            pltpu.VMEM(blocked.shape, BF16),
            pltpu.SemaphoreType.DMA((18,)),
            pltpu.SemaphoreType.DMA((18,)),
            pltpu.SemaphoreType.DMA((8,)),
        ],
        compiler_params=pltpu.CompilerParams(
            collective_id=0, has_side_effects=True, vmem_limit_bytes=VMEM_LIMIT
        ),
        name="gather_project",
    )(block, squares, blocked)


def scatter_kernel(part_ref, base_ref, out_ref, chip, x_in, y_in, x_last, y_last, send, recv):
    ctx = lax.axis_index("ctx")
    me = lax.axis_index("head")
    rows = base_ref.shape[0]
    half = half_rows(rows)
    top = pl.ds(0, half)
    low = pl.ds(half, rows - half)
    peer = [head_peer(me, flip) for flip in range(8)]
    greet([(ctx, peer[flip]) for flip in (1, 2, 4)])

    def copy(slot, flip, source, target):
        return pltpu.make_async_remote_copy(
            src_ref=source,
            dst_ref=target,
            send_sem=send.at[slot],
            recv_sem=recv.at[slot],
            device_id=(ctx, peer[flip]),
            device_id_type=MESH,
        )

    side = [copy(k, 1, part_ref.at[peer[2 * k + 1]], chip.at[k]) for k in range(4)]
    for k in (3, 1, 2, 0):
        side[k].start()

    def add_chip(k):
        side[k].wait_recv()
        chip[k] = (chip[k].astype(F32) + part_ref[peer[2 * k]].astype(F32)).astype(BF16)

    add_chip(3)
    x_far = copy(4, 2, chip.at[3, top], x_in.at[1])
    y_far = copy(5, 4, chip.at[3, low], y_in.at[1, pl.ds(0, rows - half)])
    x_far.start()
    y_far.start()
    add_chip(1)
    x_near = copy(6, 2, chip.at[1, top], x_in.at[0])
    x_near.start()
    add_chip(2)
    y_near = copy(7, 4, chip.at[2, low], y_in.at[0, pl.ds(0, rows - half)])
    y_near.start()
    side[0].wait_recv()
    x_far.wait_recv()
    chip[2, :half] = (chip[2, :half].astype(F32) + x_in[1].astype(F32)).astype(BF16)
    y_end = copy(8, 4, chip.at[2, top], y_last)
    y_end.start()
    y_far.wait_recv()
    chip[1, half:] = (
        chip[1, half:].astype(F32) + y_in[1, : rows - half].astype(F32)
    ).astype(BF16)
    x_end = copy(9, 2, chip.at[1, low], x_last.at[pl.ds(0, rows - half)])
    x_end.start()
    total = chip[0].astype(F32) + part_ref[me].astype(F32) + base_ref[...].astype(F32)
    x_near.wait_recv()
    y_near.wait_recv()
    total_top = total[:half] + x_in[0].astype(F32)
    total_low = total[half:] + y_in[0, : rows - half].astype(F32)
    y_end.wait_recv()
    out_ref[:half] = (total_top + y_last[...].astype(F32)).astype(BF16)
    x_end.wait_recv()
    out_ref[half:] = (total_low + x_last[: rows - half].astype(F32)).astype(BF16)
    for one in side + [x_far, y_far, x_near, y_near, y_end, x_end]:
        one.wait_send()


def scatter_blocks(parts, base):
    rows, width = base.shape
    half = half_rows(rows)
    return pl.pallas_call(
        scatter_kernel,
        out_shape=jax.ShapeDtypeStruct(base.shape, base.dtype),
        in_specs=[pl.BlockSpec(memory_space=pltpu.VMEM)] * 2,
        out_specs=pl.BlockSpec(memory_space=pltpu.VMEM),
        scratch_shapes=[
            pltpu.VMEM((4, rows, width), BF16),
            pltpu.VMEM((2, half, width), BF16),
            pltpu.VMEM((2, half, width), BF16),
            pltpu.VMEM((half, width), BF16),
            pltpu.VMEM((half, width), BF16),
            pltpu.SemaphoreType.DMA((10,)),
            pltpu.SemaphoreType.DMA((10,)),
        ],
        compiler_params=pltpu.CompilerParams(
            collective_id=1, has_side_effects=True, vmem_limit_bytes=VMEM_LIMIT
        ),
        name="scatter_blocks",
    )(parts, base)


def project_kernel(heads, x_ref, w_ref, rate_ref, out_ref, total):
    step = pl.program_id(0)
    for plane in range(w_ref.shape[0]):
        product = jnp.dot(x_ref[0], w_ref[plane], preferred_element_type=F32)

        @pl.when(step == 0)
        def _():
            total[plane] = product

        @pl.when(step > 0)
        def _():
            total[plane] += product

    @pl.when(step == pl.num_programs(0) - 1)
    def _():
        for plane in range(w_ref.shape[0]):
            for h in range(heads):
                out_ref[h, plane] = (
                    total[plane, :, h * HD : (h + 1) * HD] * rate_ref[...]
                ).astype(BF16)


def project(blocks, rows, weight, rate):
    planes, _, width = weight.shape
    depth = blocks.shape[2]
    heads = width // HD
    return pl.pallas_call(
        functools.partial(project_kernel, heads),
        grid=(blocks.shape[0],),
        out_shape=jax.ShapeDtypeStruct((heads, planes, rows, HD), BF16),
        in_specs=[
            pl.BlockSpec((1, rows, depth), lambda b: (b, 0, 0)),
            pl.BlockSpec((planes, depth, width), lambda b: (0, b, 0)),
            pl.BlockSpec((rows, 1), lambda b: (0, 0)),
        ],
        out_specs=pl.BlockSpec((heads, planes, rows, HD), lambda b: (0, 0, 0, 0)),
        scratch_shapes=[pltpu.VMEM((planes, rows, width), F32)],
        compiler_params=pltpu.CompilerParams(
            dimension_semantics=("arbitrary",), vmem_limit_bytes=VMEM_LIMIT
        ),
        cost_estimate=pl.CostEstimate(
            flops=2 * planes * rows * width * depth * blocks.shape[0],
            bytes_accessed=2 * planes * width * depth * blocks.shape[0],
            transcendentals=0,
        ),
        name="project",
    )(blocks, weight, rate)


def contract_last(left, right):
    return lax.dot_general(left, right, (((1,), (1,)), ((), ())), preferred_element_type=F32)


def softmax_parts(query, keys, values):
    scale = HD ** (-0.5)
    scores = [contract_last(query, key) for key in keys]
    highest = functools.reduce(
        jnp.maximum, [jnp.max(score, axis=1, keepdims=True) for score in scores]
    )
    total = 0.0
    mixed = 0.0
    for score, value in zip(scores, values):
        weight = jnp.exp2((score - highest) * (scale * math.log2(math.e)))
        total = total + jnp.sum(weight, axis=1, keepdims=True)
        mixed = mixed + jnp.dot(weight.astype(BF16), value, preferred_element_type=F32)
    return mixed, total, highest * scale


def attention_kernel(count, q_ref, *refs):
    out_ref = refs[-1]
    keys = [refs[i][0, 0] for i in range(count)]
    values = [refs[count + i][0, 0] for i in range(count)]
    mixed, total, _ = softmax_parts(q_ref[0, 0], keys, values)
    out_ref[0] = (mixed / total).astype(BF16)


def self_attention(queries, sources):
    heads, _, rows, _ = queries.shape
    tile = math.gcd(rows, 256)
    count = len(sources)
    keys_all = count * rows
    return pl.pallas_call(
        functools.partial(attention_kernel, count),
        grid=(heads, rows // tile),
        out_shape=jax.ShapeDtypeStruct((heads, rows, HD), BF16),
        in_specs=[pl.BlockSpec((1, 1, tile, HD), lambda h, i: (h, 0, i, 0))]
        + [pl.BlockSpec((1, 1, rows, HD), lambda h, i: (h, 1, 0, 0))] * count
        + [pl.BlockSpec((1, 1, rows, HD), lambda h, i: (h, 2, 0, 0))] * count,
        out_specs=pl.BlockSpec((1, tile, HD), lambda h, i: (h, i, 0)),
        compiler_params=pltpu.CompilerParams(
            dimension_semantics=("arbitrary", "arbitrary"), vmem_limit_bytes=VMEM_LIMIT
        ),
        cost_estimate=pl.CostEstimate(
            flops=8 * heads * rows * keys_all * HD,
            bytes_accessed=4 * heads * keys_all * HD,
            transcendentals=heads * rows * keys_all,
        ),
        name="self_attention",
    )(queries, *sources, *sources)


def cross_kernel(count, video_ref, *refs):
    audio = refs[:count]
    out_ref, part_ref, stats_ref = refs[count:]
    heads = video_ref.shape[0]
    for h in range(heads):
        at = [slice((plane * heads + h) * HD, (plane * heads + h + 1) * HD) for plane in range(3)]
        mixed, total, _ = softmax_parts(
            video_ref[h, 0], [one[:, at[1]] for one in audio], [one[:, at[2]] for one in audio]
        )
        out_ref[:, h * HD : (h + 1) * HD] = (mixed / total).astype(BF16)
        for d in range(count):
            mixed, total, highest = softmax_parts(
                audio[d][:, at[0]], [video_ref[h, 1]], [video_ref[h, 2]]
            )
            part_ref[d, :, h * HD : (h + 1) * HD] = (mixed / total).astype(BF16)
            lanes = lax.broadcasted_iota(jnp.int32, (mixed.shape[0], HD), 1)
            stats_ref[d, h] = jnp.where(lanes < HD // 2, total, highest)


def cross_attention(video_heads, audio_sources):
    heads, _, rows, _ = video_heads.shape
    count = len(audio_sources)
    audio_rows = audio_sources[0].shape[0]
    whole = pl.BlockSpec(memory_space=pltpu.VMEM)
    return pl.pallas_call(
        functools.partial(cross_kernel, count),
        out_shape=(
            jax.ShapeDtypeStruct((rows, heads * HD), BF16),
            jax.ShapeDtypeStruct((count, audio_rows, heads * HD), BF16),
            jax.ShapeDtypeStruct((count, heads, audio_rows, HD), F32),
        ),
        in_specs=[whole] * (1 + count),
        out_specs=(whole, whole, whole),
        compiler_params=pltpu.CompilerParams(vmem_limit_bytes=VMEM_LIMIT),
        cost_estimate=pl.CostEstimate(
            flops=16 * heads * rows * count * audio_rows * HD,
            bytes_accessed=8 * rows * heads * HD,
            transcendentals=2 * heads * rows * count * audio_rows,
        ),
        name="cross_attention",
    )(video_heads, *audio_sources)


def output_kernel(self_ref, cross_ref, audio_ref, w_self, w_cross, w_audio, out_ref):
    rows = self_ref.shape[0]
    out_ref[0, :rows] = (
        jnp.dot(self_ref[...], w_self[...], preferred_element_type=F32)
        + jnp.dot(cross_ref[...], w_cross[...], preferred_element_type=F32)
    ).astype(BF16)
    sound = jnp.dot(audio_ref[...], w_audio[...], preferred_element_type=F32).astype(BF16)
    half = sound.shape[0] // 2
    width = sound.shape[1]
    out_ref[0, rows:, :width] = sound[:half]
    out_ref[0, rows:, width:] = sound[half:]


def output_parts(self_out, cross_out, audio_out, w_self, w_cross, w_audio):
    rows, depth = self_out.shape
    audio_rows, cross_depth = audio_out.shape
    width = w_self.shape[1] // 8
    audio_width = w_audio.shape[1] // 8
    return pl.pallas_call(
        output_kernel,
        grid=(8,),
        out_shape=jax.ShapeDtypeStruct((8, rows + audio_rows // 2, width), BF16),
        in_specs=[
            pl.BlockSpec((rows, depth), lambda n: (0, 0)),
            pl.BlockSpec((rows, cross_depth), lambda n: (0, 0)),
            pl.BlockSpec((audio_rows, cross_depth), lambda n: (0, 0)),
            pl.BlockSpec((depth, width), lambda n: (0, n)),
            pl.BlockSpec((cross_depth, width), lambda n: (0, n)),
            pl.BlockSpec((cross_depth, audio_width), lambda n: (0, n)),
        ],
        out_specs=pl.BlockSpec((1, rows + audio_rows // 2, width), lambda n: (n, 0, 0)),
        compiler_params=pltpu.CompilerParams(
            dimension_semantics=("arbitrary",), vmem_limit_bytes=VMEM_LIMIT
        ),
        name="output_parts",
    )(self_out, cross_out, audio_out, w_self, w_cross, w_audio)


def pack(video_block, audio_block):
    half = audio_block.shape[0] // 2
    return jnp.concatenate(
        [video_block, jnp.concatenate([audio_block[:half], audio_block[half:]], axis=1)], axis=0
    )


def square_tile(video_squares, audio_squares):
    flat = jnp.concatenate([video_squares, audio_squares])
    size = (flat.shape[0] + 1023) // 1024 * 1024
    return jnp.pad(flat, (0, size - flat.shape[0])).reshape(-1, 128)


def fast_body(
    ctx_size,
    video,
    audio,
    video_gain,
    audio_gain,
    video_qkv,
    video_cross,
    audio_cross,
    video_out,
    cross_video_out,
    cross_audio_out,
):
    me = lax.axis_index("ctx")
    rows = video.shape[0]
    audio_rows = audio.shape[0]

    def shift(value, distance):
        ring = [(i, (i + distance) % ctx_size) for i in range(ctx_size)]
        return lax.ppermute(value, "ctx", ring)

    video_wide = video.astype(F32)
    audio_wide = audio.astype(F32)
    block = pack((video_wide * video_gain).astype(BF16), (audio_wide * audio_gain).astype(BF16))
    squares = square_tile(
        jnp.sum(video_wide * video_wide, axis=1), jnp.sum(audio_wide * audio_wide, axis=1)
    )
    blocks, every_square, self_heads = gather_project(
        block, squares, video_qkv.transpose(1, 0, 2), rows
    )
    sums = jnp.sum(every_square, axis=0).reshape(-1)
    video_rate = lax.rsqrt(sums[:rows] / video_qkv.shape[0] + EPSILON)[:, None]
    audio_rate = lax.rsqrt(sums[rows : rows + audio_rows] / audio_cross.shape[0] + EPSILON)[:, None]

    heads = self_heads.shape[0]
    shares = self_heads.reshape((ctx_size, heads // ctx_size) + self_heads.shape[1:])

    def share(stack, distance):
        return lax.dynamic_index_in_dim(stack, (me + distance) % ctx_size, 0, keepdims=False)

    outgoing = [share(shares, d) for d in range(ctx_size)]
    outgoing, blocks = lax.optimization_barrier((outgoing, blocks))
    sources = [outgoing[0]] + [shift(one, d) for d, one in enumerate(outgoing[1:2], 1)]

    audio_full = (
        blocks[:, rows:, :]
        .reshape(8, audio_rows // 2, 2, -1)
        .transpose(2, 1, 0, 3)
        .reshape(audio_rows, -1)
    )
    audio_mixed = jnp.concatenate(
        [
            (
                jnp.dot(audio_full, audio_cross[:, plane, :], preferred_element_type=F32)
                * audio_rate
            ).astype(BF16)
            for plane in range(3)
        ],
        axis=1,
    )
    later, audio_mixed = lax.optimization_barrier((outgoing[2:], audio_mixed))
    audio_sources = [audio_mixed] + [shift(audio_mixed, d) for d in range(1, ctx_size)]
    sources += [shift(one, d) for d, one in enumerate(later, 2)]
    cross_heads = project(blocks, rows, video_cross.transpose(1, 0, 2), video_rate)
    cross_out, parts, stats = cross_attention(cross_heads, audio_sources)
    own_parts = jnp.stack([parts[0]] + [shift(parts[d], -d) for d in range(1, ctx_size)])
    stats = jnp.stack([stats[..., 0], stats[..., HD - 1]], axis=1)
    own_stats = jnp.stack([stats[0]] + [shift(stats[d], -d) for d in range(1, ctx_size)])
    totals, highs = own_stats[:, 0], own_stats[:, 1]
    shares_of = totals * jnp.exp(highs - jnp.max(highs, axis=0, keepdims=True))
    shares_of = (shares_of / jnp.sum(shares_of, axis=0, keepdims=True)).transpose(0, 2, 1)
    split_parts = own_parts.astype(F32).reshape(ctx_size, audio_rows, -1, HD)
    audio_cross_out = (
        jnp.sum(split_parts * shares_of[..., None], axis=0).reshape(audio_rows, -1).astype(BF16)
    )

    results = [None] * ctx_size
    for d in list(range(1, ctx_size)) + [0]:
        result = self_attention(sources[d], sources)
        results[d] = shift(result, -d) if d else result
    doubled = jnp.concatenate(results + results, axis=0)
    group = heads // ctx_size
    ordered = lax.dynamic_slice_in_dim(
        doubled, ((ctx_size - me) % ctx_size) * group, heads, axis=0
    )
    self_out = join_heads(ordered)
    partial = output_parts(
        self_out, cross_out, audio_cross_out, video_out, cross_video_out, cross_audio_out
    )
    done = scatter_blocks(partial, pack(video, audio))
    sound = done[rows:]
    width = audio.shape[1]
    return done[:rows], jnp.concatenate([sound[:, :width], sound[:, width:]], axis=0)


def solution(mesh):
    ctx_size = mesh.shape["ctx"]

    def body(*operands):
        heads = operands[4].shape[2] // HD
        if mesh.shape["head"] == 2**3 and heads % ctx_size == 0 and operands[0].shape[0] % HD == 0:
            return fast_body(ctx_size, *operands)
        return plain_body(*operands)

    return jax.shard_map(
        body,
        mesh=mesh,
        in_specs=(
            P("ctx", "head"),
            P("ctx", "head"),
            P("head"),
            P("head"),
            P(None, None, "head"),
            P(None, None, "head"),
            P(None, None, "head"),
            P("head", None),
            P("head", None),
            P("head", None),
        ),
        out_specs=(P("ctx", "head"), P("ctx", "head")),
        check_vma=False,
    )
```

```python
import functools
import math

import jax
import jax.numpy as jnp
from jax import lax
from jax.experimental import pallas as pl
from jax.experimental.pallas import tpu as pltpu

from jax.sharding import PartitionSpec as P

HD = 128


EPSILON = 1e-06


def split_heads(matrix):
    return matrix.reshape(matrix.shape[0], -1, HD).transpose(1, 0, 2)


def join_heads(blocks):
    return blocks.transpose(1, 0, 2).reshape(blocks.shape[1], -1)


def attend(queries, keys, values):
    scale = HD ** (-0.5)

    def one_head(operands):
        query_block, key_block, value_block = operands
        scores = jnp.dot(query_block, key_block.T, preferred_element_type=jnp.float32) * scale
        highest = jnp.max(scores, axis=1, keepdims=True)
        weights = jnp.exp(scores - highest)
        totals = jnp.sum(weights, axis=1, keepdims=True)
        return (
            jnp.dot(weights.astype(jnp.bfloat16), value_block, preferred_element_type=jnp.float32)
            / totals
        )

    blocks = lax.map(one_head, (split_heads(queries), split_heads(keys), split_heads(values)))
    return join_heads(blocks).astype(jnp.bfloat16)


def plain_body(
    video,
    audio,
    video_gain,
    audio_gain,
    video_qkv,
    video_cross,
    audio_cross,
    video_out,
    cross_video_out,
    cross_audio_out,
):
    scale = HD ** (-0.5)
    video_wide = video.astype(jnp.float32)
    audio_wide = audio.astype(jnp.float32)
    video_squares, audio_squares = lax.psum(
        (jnp.sum(video_wide * video_wide, axis=1), jnp.sum(audio_wide * audio_wide, axis=1)), "head"
    )
    video_rate = lax.rsqrt(video_squares / video_qkv.shape[0] + EPSILON)
    audio_rate = lax.rsqrt(audio_squares / audio_cross.shape[0] + EPSILON)
    video_scaled = (video_wide * video_gain).astype(jnp.bfloat16)
    audio_scaled = (audio_wide * audio_gain).astype(jnp.bfloat16)
    self_weight = video_qkv.reshape(video_qkv.shape[0], -1)
    mixed_weight = video_cross.reshape(video_cross.shape[0], -1)
    audio_weight = audio_cross.reshape(audio_cross.shape[0], -1)
    self_width = video_qkv.shape[2]
    cross_width = video_cross.shape[2]
    video_rows = video.shape[0]
    segment = lax.all_gather(video_scaled, "head", axis=1, tiled=True)
    self_acc = jnp.dot(segment, self_weight, preferred_element_type=jnp.float32)
    mixed_acc = jnp.dot(segment, mixed_weight, preferred_element_type=jnp.float32)
    audio_acc = jnp.dot(
        lax.all_gather(audio_scaled, "head", axis=1, tiled=True),
        audio_weight,
        preferred_element_type=jnp.float32,
    )
    self_proj = (self_acc * video_rate[:, None]).astype(jnp.bfloat16)
    video_mixed = (mixed_acc * video_rate[:, None]).astype(jnp.bfloat16)
    audio_mixed = (audio_acc * audio_rate[:, None]).astype(jnp.bfloat16)
    query_heads = split_heads(self_proj[:, :self_width])
    local_heads = query_heads.shape[0]
    running_max = jnp.full((local_heads, video_rows), -1e30, jnp.float32)
    key_heads = split_heads(
        lax.all_gather(self_proj[:, self_width : 2 * self_width], "ctx", axis=0, tiled=True)
    )
    value_heads = split_heads(
        lax.all_gather(self_proj[:, 2 * self_width :], "ctx", axis=0, tiled=True)
    )
    scores = (
        jnp.einsum("hqd,hkd->hqk", query_heads, key_heads, preferred_element_type=jnp.float32)
        * scale
    )
    newest = jnp.maximum(running_max, jnp.max(scores, axis=2))
    weights = jnp.exp(scores - newest[:, :, None])
    running_sum = jnp.sum(weights, axis=2)
    running_acc = jnp.einsum(
        "hqk,hkd->hqd",
        weights.astype(jnp.bfloat16),
        value_heads,
        preferred_element_type=jnp.float32,
    )
    self_out = join_heads(running_acc / running_sum[:, :, None]).astype(jnp.bfloat16)
    audio_key_all, audio_value_all = (
        lax.all_gather(audio_mixed[:, cross_width : 2 * cross_width], "ctx", axis=0, tiled=True),
        lax.all_gather(audio_mixed[:, 2 * cross_width :], "ctx", axis=0, tiled=True),
    )
    video_cross_out = attend(video_mixed[:, :cross_width], audio_key_all, audio_value_all)
    queries_av = audio_mixed[:, :cross_width]
    keys_av = video_mixed[:, cross_width : 2 * cross_width]
    values_av = video_mixed[:, 2 * cross_width :]
    every_query = lax.all_gather(queries_av, "ctx", axis=0, tiled=True)
    scores = (
        jnp.einsum(
            "hqd,hkd->hqk",
            split_heads(every_query),
            split_heads(keys_av),
            preferred_element_type=jnp.float32,
        )
        * scale
    )
    highest = lax.pmax(jnp.max(scores, axis=2), "ctx")
    weights = jnp.exp(scores - highest[:, :, None])
    numerators = jnp.einsum(
        "hqk,hkd->hqd",
        weights.astype(jnp.bfloat16),
        split_heads(values_av),
        preferred_element_type=jnp.float32,
    )
    weight_totals = jnp.sum(weights, axis=2)
    own_numer, own_totals = (
        lax.psum_scatter(
            numerators.astype(jnp.bfloat16), "ctx", scatter_dimension=1, tiled=True
        ).astype(jnp.float32),
        lax.psum_scatter(
            weight_totals.astype(jnp.bfloat16), "ctx", scatter_dimension=1, tiled=True
        ).astype(jnp.float32),
    )
    audio_cross_out = join_heads(own_numer / own_totals[:, :, None]).astype(jnp.bfloat16)
    video_partial = jnp.dot(self_out, video_out, preferred_element_type=jnp.float32) + jnp.dot(
        video_cross_out, cross_video_out, preferred_element_type=jnp.float32
    )
    audio_partial = jnp.dot(audio_cross_out, cross_audio_out, preferred_element_type=jnp.float32)
    video_sum, audio_sum = (
        lax.psum_scatter(
            video_partial.astype(jnp.bfloat16), "head", scatter_dimension=1, tiled=True
        ).astype(jnp.float32),
        lax.psum_scatter(
            audio_partial.astype(jnp.bfloat16), "head", scatter_dimension=1, tiled=True
        ).astype(jnp.float32),
    )
    return (
        (video_wide + video_sum).astype(jnp.bfloat16),
        (audio_wide + audio_sum).astype(jnp.bfloat16),
    )


MESH = pl.DeviceIdType.MESH
F32 = jnp.float32
BF16 = jnp.bfloat16
VMEM_LIMIT = 60 * 1024 * 1024


def greet(peers):
    barrier = pltpu.get_barrier_semaphore()
    for peer in peers:
        pl.semaphore_signal(barrier, inc=1, device_id=peer, device_id_type=MESH)
    pl.semaphore_wait(barrier, len(peers))


def head_peer(me, flip):
    low = me % 2
    mid = (me // 2) % 2
    high = me // 4
    if flip & 1:
        low = 1 - low
    if flip & 2:
        mid = 1 - mid
    if flip & 4:
        high = 1 - high
    return high * 4 + mid * 2 + low


def half_rows(rows):
    return (rows // 2 + 15) // 16 * 16


def gather_kernel(
    x_ref, sq_ref, w_ref, out_ref, sqs_ref, heads_ref, total, weights, send, recv, load
):
    ctx = lax.axis_index("ctx")
    me = lax.axis_index("head")
    rows = x_ref.shape[0]
    half = half_rows(rows)
    top = pl.ds(0, half)
    low = pl.ds(half, rows - half)
    peer = [head_peer(me, flip) for flip in range(8)]
    order = (0, 1, 2, 4, 3, 5, 6, 7)
    loads = {
        flip: pltpu.make_async_copy(w_ref.at[:, peer[flip]], weights.at[:, peer[flip]], load.at[flip])
        for flip in order
    }
    for flip in order:
        loads[flip].start()
    greet([(ctx, peer[flip]) for flip in range(1, 8)])

    def copy(slot, flip, source, target):
        return pltpu.make_async_remote_copy(
            src_ref=source,
            dst_ref=target,
            send_sem=send.at[slot],
            recv_sem=recv.at[slot],
            device_id=(ctx, peer[flip]),
            device_id_type=MESH,
        )

    squares = [copy(10 + flip, flip, sq_ref, sqs_ref.at[flip]) for flip in range(1, 8)]
    x_top = copy(0, 2, x_ref.at[top], out_ref.at[me, top])
    x_low = copy(1, 2, x_ref.at[low], out_ref.at[me, low])
    y_low = copy(2, 4, x_ref.at[low], out_ref.at[me, low])
    y_top = copy(3, 4, x_ref.at[top], out_ref.at[me, top])
    side = copy(4, 1, x_ref, out_ref.at[me])
    x_top.start()
    y_low.start()
    x_low.start()
    y_top.start()
    side.start()
    for square in squares:
        square.start()

    planes, tokens, width = total.shape
    tile = math.gcd(tokens, 256)
    tiles = tokens // tile

    def multiply(flip):
        loads[flip].wait()

        def step(i, carry):
            plane = i // tiles
            at = pl.ds(pl.multiple_of((i % tiles) * tile, tile), tile)
            product = jnp.dot(
                out_ref[peer[flip], at], weights[plane, peer[flip]], preferred_element_type=F32
            )
            total[plane, at] = product if flip == 0 else total[plane, at] + product
            return carry

        lax.fori_loop(0, planes * tiles, step, 0)

    out_ref[me] = x_ref[...]
    sqs_ref[0] = sq_ref[...]
    multiply(0)
    side.wait_recv()
    multiply(1)
    from_x = peer[2]
    from_y = peer[4]
    far = peer[6]
    x_top.wait_recv()
    far_top = copy(5, 4, out_ref.at[from_x, top], out_ref.at[from_x, top])
    far_top.start()
    y_low.wait_recv()
    far_low = copy(6, 2, out_ref.at[from_y, low], out_ref.at[from_y, low])
    far_low.start()
    x_low.wait_recv()
    side_x = copy(7, 1, out_ref.at[from_x], out_ref.at[from_x])
    side_x.start()
    y_top.wait_recv()
    side_y = copy(8, 1, out_ref.at[from_y], out_ref.at[from_y])
    side_y.start()
    multiply(2)
    multiply(4)
    side_x.wait_recv()
    multiply(3)
    side_y.wait_recv()
    multiply(5)
    far_top.wait_recv()
    side_top = copy(9, 1, out_ref.at[far, top], out_ref.at[far, top])
    side_top.start()
    far_low.wait_recv()
    side_low = copy(10, 1, out_ref.at[far, low], out_ref.at[far, low])
    side_low.start()
    multiply(6)
    side_top.wait_recv()
    side_low.wait_recv()
    multiply(7)
    for square in squares:
        square.wait_recv()
    sums = jnp.sum(sqs_ref[...], axis=0)
    rate_rows = lax.rsqrt(sums / (8 * x_ref.shape[1]) + EPSILON)
    line = lax.broadcasted_iota(jnp.int32, (HD, HD), 0)
    lane = lax.broadcasted_iota(jnp.int32, (HD, HD), 1)
    for piece in range(tokens // HD):
        spread = jnp.broadcast_to(rate_rows[piece : piece + 1], (HD, HD))
        rate = jnp.sum(jnp.where(line == lane, spread, 0.0), axis=1, keepdims=True)
        at = slice(piece * HD, (piece + 1) * HD)
        for plane in range(planes):
            scaled = (total[plane, at] * rate).astype(BF16)
            for h in range(width // HD):
                heads_ref[h, plane, at] = scaled[:, h * HD : (h + 1) * HD]
    for one in squares + [
        x_top, x_low, y_low, y_top, side, far_top, far_low, side_x, side_y, side_top, side_low
    ]:
        one.wait_send()


def gather_project(block, squares, weight, tokens):
    planes, depth, width = weight.shape
    vmem = pl.BlockSpec(memory_space=pltpu.VMEM)
    blocked = weight.reshape(planes, 8, depth // 8, width)
    return pl.pallas_call(
        gather_kernel,
        out_shape=(
            jax.ShapeDtypeStruct((8,) + block.shape, block.dtype),
            jax.ShapeDtypeStruct((8,) + squares.shape, squares.dtype),
            jax.ShapeDtypeStruct((width // HD, planes, tokens, HD), BF16),
        ),
        in_specs=[vmem, vmem, pl.BlockSpec(memory_space=pl.ANY)],
        out_specs=(vmem, vmem, vmem),
        scratch_shapes=[
            pltpu.VMEM((planes, tokens, width), F32),
            pltpu.VMEM(blocked.shape, BF16),
            pltpu.SemaphoreType.DMA((18,)),
            pltpu.SemaphoreType.DMA((18,)),
            pltpu.SemaphoreType.DMA((8,)),
        ],
        compiler_params=pltpu.CompilerParams(
            collective_id=0, has_side_effects=True, vmem_limit_bytes=VMEM_LIMIT
        ),
        name="gather_project",
    )(block, squares, blocked)


def scatter_kernel(part_ref, base_ref, out_ref, chip, x_in, y_in, x_last, y_last, send, recv):
    ctx = lax.axis_index("ctx")
    me = lax.axis_index("head")
    rows = base_ref.shape[0]
    half = half_rows(rows)
    top = pl.ds(0, half)
    low = pl.ds(half, rows - half)
    peer = [head_peer(me, flip) for flip in range(8)]
    greet([(ctx, peer[flip]) for flip in (1, 2, 4)])

    def copy(slot, flip, source, target):
        return pltpu.make_async_remote_copy(
            src_ref=source,
            dst_ref=target,
            send_sem=send.at[slot],
            recv_sem=recv.at[slot],
            device_id=(ctx, peer[flip]),
            device_id_type=MESH,
        )

    side = [copy(k, 1, part_ref.at[peer[2 * k + 1]], chip.at[k]) for k in range(4)]
    for k in (3, 1, 2, 0):
        side[k].start()

    def add_chip(k):
        side[k].wait_recv()
        chip[k] = (chip[k].astype(F32) + part_ref[peer[2 * k]].astype(F32)).astype(BF16)

    add_chip(3)
    x_far = copy(4, 2, chip.at[3, top], x_in.at[1])
    y_far = copy(5, 4, chip.at[3, low], y_in.at[1, pl.ds(0, rows - half)])
    x_far.start()
    y_far.start()
    add_chip(1)
    x_near = copy(6, 2, chip.at[1, top], x_in.at[0])
    x_near.start()
    add_chip(2)
    y_near = copy(7, 4, chip.at[2, low], y_in.at[0, pl.ds(0, rows - half)])
    y_near.start()
    side[0].wait_recv()
    x_far.wait_recv()
    chip[2, :half] = (chip[2, :half].astype(F32) + x_in[1].astype(F32)).astype(BF16)
    y_end = copy(8, 4, chip.at[2, top], y_last)
    y_end.start()
    y_far.wait_recv()
    chip[1, half:] = (
        chip[1, half:].astype(F32) + y_in[1, : rows - half].astype(F32)
    ).astype(BF16)
    x_end = copy(9, 2, chip.at[1, low], x_last.at[pl.ds(0, rows - half)])
    x_end.start()
    total = chip[0].astype(F32) + part_ref[me].astype(F32) + base_ref[...].astype(F32)
    x_near.wait_recv()
    y_near.wait_recv()
    total_top = total[:half] + x_in[0].astype(F32)
    total_low = total[half:] + y_in[0, : rows - half].astype(F32)
    y_end.wait_recv()
    out_ref[:half] = (total_top + y_last[...].astype(F32)).astype(BF16)
    x_end.wait_recv()
    out_ref[half:] = (total_low + x_last[: rows - half].astype(F32)).astype(BF16)
    for one in side + [x_far, y_far, x_near, y_near, y_end, x_end]:
        one.wait_send()


def scatter_blocks(parts, base):
    rows, width = base.shape
    half = half_rows(rows)
    return pl.pallas_call(
        scatter_kernel,
        out_shape=jax.ShapeDtypeStruct(base.shape, base.dtype),
        in_specs=[pl.BlockSpec(memory_space=pltpu.VMEM)] * 2,
        out_specs=pl.BlockSpec(memory_space=pltpu.VMEM),
        scratch_shapes=[
            pltpu.VMEM((4, rows, width), BF16),
            pltpu.VMEM((2, half, width), BF16),
            pltpu.VMEM((2, half, width), BF16),
            pltpu.VMEM((half, width), BF16),
            pltpu.VMEM((half, width), BF16),
            pltpu.SemaphoreType.DMA((10,)),
            pltpu.SemaphoreType.DMA((10,)),
        ],
        compiler_params=pltpu.CompilerParams(
            collective_id=1, has_side_effects=True, vmem_limit_bytes=VMEM_LIMIT
        ),
        name="scatter_blocks",
    )(parts, base)


def project_kernel(heads, x_ref, w_ref, rate_ref, out_ref, total):
    step = pl.program_id(0)
    for plane in range(w_ref.shape[0]):
        product = jnp.dot(x_ref[0], w_ref[plane], preferred_element_type=F32)

        @pl.when(step == 0)
        def _():
            total[plane] = product

        @pl.when(step > 0)
        def _():
            total[plane] += product

    @pl.when(step == pl.num_programs(0) - 1)
    def _():
        for plane in range(w_ref.shape[0]):
            for h in range(heads):
                out_ref[h, plane] = (
                    total[plane, :, h * HD : (h + 1) * HD] * rate_ref[...]
                ).astype(BF16)


def project(blocks, rows, weight, rate):
    planes, _, width = weight.shape
    depth = blocks.shape[2]
    heads = width // HD
    return pl.pallas_call(
        functools.partial(project_kernel, heads),
        grid=(blocks.shape[0],),
        out_shape=jax.ShapeDtypeStruct((heads, planes, rows, HD), BF16),
        in_specs=[
            pl.BlockSpec((1, rows, depth), lambda b: (b, 0, 0)),
            pl.BlockSpec((planes, depth, width), lambda b: (0, b, 0)),
            pl.BlockSpec((rows, 1), lambda b: (0, 0)),
        ],
        out_specs=pl.BlockSpec((heads, planes, rows, HD), lambda b: (0, 0, 0, 0)),
        scratch_shapes=[pltpu.VMEM((planes, rows, width), F32)],
        compiler_params=pltpu.CompilerParams(
            dimension_semantics=("arbitrary",), vmem_limit_bytes=VMEM_LIMIT
        ),
        cost_estimate=pl.CostEstimate(
            flops=2 * planes * rows * width * depth * blocks.shape[0],
            bytes_accessed=2 * planes * width * depth * blocks.shape[0],
            transcendentals=0,
        ),
        name="project",
    )(blocks, weight, rate)


def contract_last(left, right):
    return lax.dot_general(left, right, (((1,), (1,)), ((), ())), preferred_element_type=F32)


def softmax_parts(query, keys, values):
    scale = HD ** (-0.5)
    scores = [contract_last(query, key) for key in keys]
    highest = functools.reduce(
        jnp.maximum, [jnp.max(score, axis=1, keepdims=True) for score in scores]
    )
    total = 0.0
    mixed = 0.0
    for score, value in zip(scores, values):
        weight = jnp.exp2((score - highest) * (scale * math.log2(math.e)))
        total = total + jnp.sum(weight, axis=1, keepdims=True)
        mixed = mixed + jnp.dot(weight.astype(BF16), value, preferred_element_type=F32)
    return mixed, total, highest * scale


def attention_kernel(count, q_ref, *refs):
    out_ref = refs[-1]
    keys = [refs[i][0, 0] for i in range(count)]
    values = [refs[count + i][0, 0] for i in range(count)]
    mixed, total, _ = softmax_parts(q_ref[0, 0], keys, values)
    out_ref[0] = (mixed / total).astype(BF16)


def self_attention(queries, sources):
    heads, _, rows, _ = queries.shape
    tile = math.gcd(rows, 256)
    count = len(sources)
    keys_all = count * rows
    return pl.pallas_call(
        functools.partial(attention_kernel, count),
        grid=(heads, rows // tile),
        out_shape=jax.ShapeDtypeStruct((heads, rows, HD), BF16),
        in_specs=[pl.BlockSpec((1, 1, tile, HD), lambda h, i: (h, 0, i, 0))]
        + [pl.BlockSpec((1, 1, rows, HD), lambda h, i: (h, 1, 0, 0))] * count
        + [pl.BlockSpec((1, 1, rows, HD), lambda h, i: (h, 2, 0, 0))] * count,
        out_specs=pl.BlockSpec((1, tile, HD), lambda h, i: (h, i, 0)),
        compiler_params=pltpu.CompilerParams(
            dimension_semantics=("arbitrary", "arbitrary"), vmem_limit_bytes=VMEM_LIMIT
        ),
        cost_estimate=pl.CostEstimate(
            flops=8 * heads * rows * keys_all * HD,
            bytes_accessed=4 * heads * keys_all * HD,
            transcendentals=heads * rows * keys_all,
        ),
        name="self_attention",
    )(queries, *sources, *sources)


def cross_kernel(count, video_ref, *refs):
    audio = refs[:count]
    out_ref, part_ref, stats_ref = refs[count:]
    heads = video_ref.shape[0]
    for h in range(heads):
        at = [slice((plane * heads + h) * HD, (plane * heads + h + 1) * HD) for plane in range(3)]
        mixed, total, _ = softmax_parts(
            video_ref[h, 0], [one[:, at[1]] for one in audio], [one[:, at[2]] for one in audio]
        )
        out_ref[:, h * HD : (h + 1) * HD] = (mixed / total).astype(BF16)
        for d in range(count):
            mixed, total, highest = softmax_parts(
                audio[d][:, at[0]], [video_ref[h, 1]], [video_ref[h, 2]]
            )
            part_ref[d, :, h * HD : (h + 1) * HD] = (mixed / total).astype(BF16)
            lanes = lax.broadcasted_iota(jnp.int32, (mixed.shape[0], HD), 1)
            stats_ref[d, h] = jnp.where(lanes < HD // 2, total, highest)


def cross_attention(video_heads, audio_sources):
    heads, _, rows, _ = video_heads.shape
    count = len(audio_sources)
    audio_rows = audio_sources[0].shape[0]
    whole = pl.BlockSpec(memory_space=pltpu.VMEM)
    return pl.pallas_call(
        functools.partial(cross_kernel, count),
        out_shape=(
            jax.ShapeDtypeStruct((rows, heads * HD), BF16),
            jax.ShapeDtypeStruct((count, audio_rows, heads * HD), BF16),
            jax.ShapeDtypeStruct((count, heads, audio_rows, HD), F32),
        ),
        in_specs=[whole] * (1 + count),
        out_specs=(whole, whole, whole),
        compiler_params=pltpu.CompilerParams(vmem_limit_bytes=VMEM_LIMIT),
        cost_estimate=pl.CostEstimate(
            flops=16 * heads * rows * count * audio_rows * HD,
            bytes_accessed=8 * rows * heads * HD,
            transcendentals=2 * heads * rows * count * audio_rows,
        ),
        name="cross_attention",
    )(video_heads, *audio_sources)


def output_kernel(self_ref, cross_ref, audio_ref, w_self, w_cross, w_audio, out_ref):
    rows = self_ref.shape[0]
    out_ref[0, :rows] = (
        jnp.dot(self_ref[...], w_self[...], preferred_element_type=F32)
        + jnp.dot(cross_ref[...], w_cross[...], preferred_element_type=F32)
    ).astype(BF16)
    sound = jnp.dot(audio_ref[...], w_audio[...], preferred_element_type=F32).astype(BF16)
    half = sound.shape[0] // 2
    width = sound.shape[1]
    out_ref[0, rows:, :width] = sound[:half]
    out_ref[0, rows:, width:] = sound[half:]


def output_parts(self_out, cross_out, audio_out, w_self, w_cross, w_audio):
    rows, depth = self_out.shape
    audio_rows, cross_depth = audio_out.shape
    width = w_self.shape[1] // 8
    audio_width = w_audio.shape[1] // 8
    return pl.pallas_call(
        output_kernel,
        grid=(8,),
        out_shape=jax.ShapeDtypeStruct((8, rows + audio_rows // 2, width), BF16),
        in_specs=[
            pl.BlockSpec((rows, depth), lambda n: (0, 0)),
            pl.BlockSpec((rows, cross_depth), lambda n: (0, 0)),
            pl.BlockSpec((audio_rows, cross_depth), lambda n: (0, 0)),
            pl.BlockSpec((depth, width), lambda n: (0, n)),
            pl.BlockSpec((cross_depth, width), lambda n: (0, n)),
            pl.BlockSpec((cross_depth, audio_width), lambda n: (0, n)),
        ],
        out_specs=pl.BlockSpec((1, rows + audio_rows // 2, width), lambda n: (n, 0, 0)),
        compiler_params=pltpu.CompilerParams(
            dimension_semantics=("arbitrary",), vmem_limit_bytes=VMEM_LIMIT
        ),
        name="output_parts",
    )(self_out, cross_out, audio_out, w_self, w_cross, w_audio)


def pack(video_block, audio_block):
    half = audio_block.shape[0] // 2
    return jnp.concatenate(
        [video_block, jnp.concatenate([audio_block[:half], audio_block[half:]], axis=1)], axis=0
    )


def square_tile(video_squares, audio_squares):
    flat = jnp.concatenate([video_squares, audio_squares])
    size = (flat.shape[0] + 1023) // 1024 * 1024
    return jnp.pad(flat, (0, size - flat.shape[0])).reshape(-1, 128)


def fast_body(
    ctx_size,
    video,
    audio,
    video_gain,
    audio_gain,
    video_qkv,
    video_cross,
    audio_cross,
    video_out,
    cross_video_out,
    cross_audio_out,
):
    me = lax.axis_index("ctx")
    rows = video.shape[0]
    audio_rows = audio.shape[0]

    def shift(value, distance):
        ring = [(i, (i + distance) % ctx_size) for i in range(ctx_size)]
        return lax.ppermute(value, "ctx", ring)

    video_wide = video.astype(F32)
    audio_wide = audio.astype(F32)
    block = pack((video_wide * video_gain).astype(BF16), (audio_wide * audio_gain).astype(BF16))
    squares = square_tile(
        jnp.sum(video_wide * video_wide, axis=1), jnp.sum(audio_wide * audio_wide, axis=1)
    )
    blocks, every_square, self_heads = gather_project(
        block, squares, video_qkv.transpose(1, 0, 2), rows
    )
    sums = jnp.sum(every_square, axis=0).reshape(-1)
    video_rate = lax.rsqrt(sums[:rows] / video_qkv.shape[0] + EPSILON)[:, None]
    audio_rate = lax.rsqrt(sums[rows : rows + audio_rows] / audio_cross.shape[0] + EPSILON)[:, None]

    heads = self_heads.shape[0]
    shares = self_heads.reshape((ctx_size, heads // ctx_size) + self_heads.shape[1:])

    def share(stack, distance):
        return lax.dynamic_index_in_dim(stack, (me + distance) % ctx_size, 0, keepdims=False)

    outgoing = [share(shares, d) for d in range(ctx_size)]
    outgoing, blocks = lax.optimization_barrier((outgoing, blocks))
    sources = [outgoing[0]] + [shift(one, d) for d, one in enumerate(outgoing[1:2], 1)]

    audio_full = (
        blocks[:, rows:, :]
        .reshape(8, audio_rows // 2, 2, -1)
        .transpose(2, 1, 0, 3)
        .reshape(audio_rows, -1)
    )
    audio_planes = [
        (
            jnp.dot(audio_full, audio_cross[:, plane, :], preferred_element_type=F32)
            * audio_rate
        ).astype(BF16)
        for plane in range(3)
    ]
    audio_mixed = jnp.concatenate(audio_planes, axis=1)
    later, audio_mixed = lax.optimization_barrier((outgoing[2:], audio_mixed))
    audio_sources = [audio_mixed] + [shift(audio_mixed, d) for d in range(1, ctx_size)]
    sources += [shift(one, d) for d, one in enumerate(later, 2)]
    cross_heads = project(blocks, rows, video_cross.transpose(1, 0, 2), video_rate)
    cross_out, parts, stats = cross_attention(cross_heads, audio_sources)
    own_parts = jnp.stack([parts[0]] + [shift(parts[d], -d) for d in range(1, ctx_size)])
    stats = jnp.stack([stats[..., 0], stats[..., HD - 1]], axis=1)
    own_stats = jnp.stack([stats[0]] + [shift(stats[d], -d) for d in range(1, ctx_size)])
    totals, highs = own_stats[:, 0], own_stats[:, 1]
    shares_of = totals * jnp.exp(highs - jnp.max(highs, axis=0, keepdims=True))
    shares_of = (shares_of / jnp.sum(shares_of, axis=0, keepdims=True)).transpose(0, 2, 1)
    split_parts = own_parts.astype(F32).reshape(ctx_size, audio_rows, -1, HD)
    audio_cross_out = (
        jnp.sum(split_parts * shares_of[..., None], axis=0).reshape(audio_rows, -1).astype(BF16)
    )

    results = [None] * ctx_size
    for d in list(range(1, ctx_size)) + [0]:
        result = self_attention(sources[d], sources)
        results[d] = shift(result, -d) if d else result
    doubled = jnp.concatenate(results + results, axis=0)
    group = heads // ctx_size
    ordered = lax.dynamic_slice_in_dim(
        doubled, ((ctx_size - me) % ctx_size) * group, heads, axis=0
    )
    self_out = join_heads(ordered)
    partial = output_parts(
        self_out, cross_out, audio_cross_out, video_out, cross_video_out, cross_audio_out
    )
    done = scatter_blocks(partial, pack(video, audio))
    sound = done[rows:]
    width = audio.shape[1]
    return done[:rows], jnp.concatenate([sound[:, :width], sound[:, width:]], axis=0)


def solution(mesh):
    ctx_size = mesh.shape["ctx"]

    def body(*operands):
        heads = operands[4].shape[2] // HD
        if mesh.shape["head"] == 2**3 and heads % ctx_size == 0 and operands[0].shape[0] % HD == 0:
            return fast_body(ctx_size, *operands)
        return plain_body(*operands)

    return jax.shard_map(
        body,
        mesh=mesh,
        in_specs=(
            P("ctx", "head"),
            P("ctx", "head"),
            P("head"),
            P("head"),
            P(None, None, "head"),
            P(None, None, "head"),
            P(None, None, "head"),
            P("head", None),
            P("head", None),
            P("head", None),
        ),
        out_specs=(P("ctx", "head"), P("ctx", "head")),
        check_vma=False,
    )
```
